32 devices in a mesh: docs: 8 (over z, x), topics: 4 (over y, core).
Axes of the slice: x: 2, y: 2, z: 4, core: 2. Of those that a mesh axis runs over, the one named last changes fastest.
Arguments:
- log_beta: bfloat16 [262144, 2048], P('docs', 'topics'), may hold values from -250 to -4
- gamma_init: float32 [128, 2048], P('docs', 'topics'), may hold values from 0.05 to 5
- topic_prior: float32 [2048], P('topics'), may hold values from 0.02 to 0.5
- word_block: int32 [128, 256, 1], P('docs'), may hold values from 0 to 7; in each aligned block of 4096 rows (0 to 4095, 4096 to 8191, ..., all dimensions but the last counted through in order) at most 1024 rows name the same one
- word_row: int32 [128, 256], P('docs'), may hold values from 0 to 32767
- counts: int32 [128, 256], P('docs'), may hold values from 0 to 2
Outputs:
- doc_gamma: float32 [128, 2048], P('docs', 'topics')
- sstats: float32 [262144, 2048], P('docs', 'topics')
The draws below stay inside these ranges and needn't reach their ends.
Inputs may be any that keep to these rules, and one draw needn't show every extreme that they name: `word_block`: among the token slots of one device's 16 documents, at most 1024 name the same vocabulary block, and some block is named by exactly 1024 of them on some device. `counts`: A count of 0 marks an empty slot.
All inputs are finite; a program needn't handle non-finite values.
Results may differ from the reference program's by a relative error of at most 0.0003.
Values may be sent and summed in bfloat16 or wider, within the bound.
A program may use at most 192 MiB of HBM per device.

```python
import math
import jax
import jax.numpy as jnp
import numpy as np
from jax import lax

K = 2048
VOCAB = 262144
LEN = 256
ITERS = 3
DOC_DEV = 16
DOCS = 128
VOC_DEV = 32768
CAP = 1024
N_DOCS = 8


def draw_log_beta(key, part):
    values = jax.random.uniform(key, (VOCAB, K), jnp.float32, -14.0, -4.0)
    return values.astype(jnp.bfloat16)


def place_ends(result, key, least, largest):
    spot = [jax.random.randint(jax.random.fold_in(key, axis), (), 0, length) for axis, length in enumerate(result.shape)]
    widest = result.shape.index(max(result.shape))
    beside = spot[:widest] + [(spot[widest] + 1) % result.shape[widest]] + spot[widest + 1:]
    return result.at[tuple(spot)].set(least).at[tuple(beside)].set(largest)


def levels(key, extent, cuts, low, top_value):
    level, own = 1.0, jax.random.fold_in(key, 6)
    for dim, parts in cuts:
        heights = jnp.exp(jax.random.uniform(jax.random.fold_in(own, dim), (parts,), jnp.float32, low / len(cuts), top_value / len(cuts)))
        level = level * jnp.repeat(heights, extent[dim] // parts).reshape([-1 if axis == dim else 1 for axis in range(len(extent))])
    return level


def assign_block(rng, own, number, rows, count, top, bound, slope):
    order = jax.random.permutation(rng, count)
    packed, common = load_shares(count, rows * top, bound, slope, True), load_shares(count, rows * top, bound, slope, False)
    places = jnp.arange(count)

    def named(lengths, offset_by):
        used = int((lengths > 0).sum())
        fixed = max(1, used // 4)
        shifted = fixed + (places - fixed + offset_by * (used - fixed)) % max(1, count - fixed)
        return jnp.zeros((count,), jnp.int32).at[order[jnp.where(places < fixed, places, shifted)]].set(jnp.asarray(lengths, jnp.int32))

    lengths = jnp.where(number % 4 == 0, named(packed, number // 4), named(common, number - number // 4 - 1))
    mixed = jax.random.permutation(jax.random.fold_in(own, 3), count)
    source_of, receiver = mixed[0:count // 2 * 2:2], mixed[1:count // 2 * 2:2]
    room = jnp.minimum(lengths[source_of] - 1, bound - lengths[receiver]) // 2
    room = jnp.where((source_of == order[0]) | (receiver == order[0]) | (lengths[receiver] == 0), 0, jnp.maximum(room, 0))
    shifted = jax.random.randint(jax.random.fold_in(own, 4), (count // 2,), 0, 1 << 20) % (room + 1)
    lengths = lengths.at[source_of].add(-shifted).at[receiver].add(shifted)
    labels = jnp.searchsorted(jnp.cumsum(lengths), jnp.arange(rows * top), side="right").astype(jnp.int32)
    listing = labels.reshape(top, rows).T
    listing = listing[jax.random.permutation(jax.random.fold_in(own, 1), rows)]
    offset_by = jax.random.randint(jax.random.fold_in(own, 2), (rows, 1), 0, top)
    return jnp.take_along_axis(listing, (jnp.arange(top)[None, :] + offset_by) % top, axis=1)


def load_shares(number_of, total, bound, skew, full):
    weights = [(1 << 20) // math.isqrt(standing ** skew) + 1 for standing in range(1, number_of + 1)]
    largest = bound if full else min(bound, max(-(-total // number_of), total * weights[0] // sum(weights)))
    least = 1 if total - largest >= number_of - 1 else 0
    given, rest = [largest] + [least] * (number_of - 1), total - largest - least * (number_of - 1)
    while rest > 0:
        free = [i for i in range(1, number_of) if given[i] < largest] or [i for i in range(1, number_of) if given[i] < bound]
        pool, budget = sum([weights[i] for i in free]), rest
        for i in free:
            addition = min(bound - given[i], max(1, budget * weights[i] // pool), rest)
            given[i] = given[i] + addition
            rest = rest - addition
    return np.array(given)


def setup_inputs(seed: int = 0) -> dict:
    splits = jax.random.split(jax.random.key(seed), 7)
    log_beta = draw_log_beta(jax.random.fold_in(splits[6], 71), 0)
    gamma_init = jnp.clip(jnp.exp(math.log(5.0) - 4.6051702 * jax.random.uniform(splits[1], (DOCS, K), jnp.float32) ** levels(splits[1], (DOCS, K), ((0, 8), (1, 4)), -0.2, 0.2)), 0.05, 5.0)
    topic_prior = jnp.clip(jnp.exp(math.log(0.5) - 3.218876 * jax.random.uniform(splits[2], (K,), jnp.float32) ** levels(splits[2], (K,), ((0, 4),), -0.2, 0.2)), 0.02, 0.5)
    word_block_keys = jax.random.split(jax.random.fold_in(splits[3], 1), DOCS * LEN // (DOC_DEV * LEN))
    word_block_turns = jax.random.permutation(jax.random.fold_in(splits[3], 3), DOCS * LEN // (DOC_DEV * LEN))
    word_block = jax.vmap(lambda own, number: assign_block(jax.random.fold_in(splits[3], 2), own, number, DOC_DEV * LEN, N_DOCS, 1, CAP, 1))(word_block_keys, word_block_turns).reshape((DOCS, LEN, 1))
    word_row = place_ends(jax.random.randint(splits[4], (DOCS, LEN), 0, VOC_DEV), jax.random.fold_in(splits[4], 1), 0, VOC_DEV - 1).astype(jnp.int32)
    counts = place_ends(jax.random.randint(splits[5], (DOCS, LEN), 0, 3), jax.random.fold_in(splits[5], 1), 0, 2).astype(jnp.int32)
    return {"log_beta": log_beta, "gamma_init": gamma_init, "topic_prior": topic_prior, "word_block": word_block, "word_row": word_row, "counts": counts}


def expect_log(doc_gamma):
    return lax.digamma(doc_gamma)


def token_weights(log_theta, beta_rows):
    scores = log_theta[:, None, :] + beta_rows.astype(jnp.float32)
    row_max = jnp.max(scores, axis=2)
    exp_mass = jnp.sum(jnp.exp(scores - row_max[:, :, None]), axis=2)
    log_norm = row_max + jnp.log(exp_mass)
    return jnp.exp(scores - log_norm[:, :, None])


def reference(log_beta, gamma_init, topic_prior, word_block, word_row, counts):
    word_ids = word_block[:, :, 0] * VOC_DEV + word_row
    word_sets = word_ids.reshape(N_DOCS, DOC_DEV, LEN)
    count_sets = counts.astype(jnp.float32).reshape(N_DOCS, DOC_DEV, LEN)
    doc_gamma = gamma_init
    for sweep_index in range(ITERS):
        log_theta = expect_log(doc_gamma).reshape(N_DOCS, DOC_DEV, K)

        def renew_block(pieces):
            theta_part, word_part, count_part = pieces
            topic_share = token_weights(theta_part, log_beta[word_part])
            return topic_prior[None, :] + jnp.einsum("dn,dnk->dk", count_part, topic_share, precision=lax.Precision.HIGHEST)

        doc_gamma = lax.map(renew_block, (log_theta, word_sets, count_sets)).reshape(DOCS, K)
    final_theta = expect_log(doc_gamma).reshape(N_DOCS, DOC_DEV, K)

    def accumulate(doc_block, sstats):
        word_part = word_sets[doc_block]
        topic_share = token_weights(final_theta[doc_block], log_beta[word_part])
        contrib = count_sets[doc_block][:, :, None] * topic_share
        return sstats.at[word_part.reshape(-1)].add(contrib.reshape(-1, K))

    sstats = lax.fori_loop(0, N_DOCS, accumulate, jnp.zeros((VOCAB, K), jnp.float32))
    return doc_gamma, sstats
```

```python
import functools

import jax
import jax.numpy as jnp
from jax import lax
from jax.experimental import pallas as pl
from jax.experimental.pallas import tpu as pltpu
from jax.sharding import PartitionSpec as P

ITERS = 3
MESH = pl.DeviceIdType.MESH
LANES = 256
DEEP = 2048
PIECE = 128
SUB = 256
STEP = 16
HALVES = 2
GATHER_LIMIT = 16 * 1024 * 1024
SWEEP_LIMIT = 12 * 1024 * 1024
STATS_LIMIT = 16 * 1024 * 1024


def share_kernel(owners, vocab, packed_ref, key_ref, seen, send, recv):
    me, part = lax.axis_index("docs"), lax.axis_index("topics")
    doc_rows = packed_ref.shape[0]
    all_docs = owners * doc_rows

    def owner(i):
        return lax.rem(me + i, owners)

    barrier = pltpu.get_barrier_semaphore()
    for i in range(1, owners):
        pl.semaphore_signal(barrier, inc=1, device_id=(owner(i), part), device_id_type=MESH)
    pl.semaphore_wait(barrier, owners - 1)

    def copy(i):
        return pltpu.make_async_remote_copy(
            src_ref=packed_ref, dst_ref=seen.at[me], send_sem=send.at[i], recv_sem=recv.at[i],
            device_id=(owner(i), part), device_id_type=MESH,
        )

    for i in range(1, owners):
        copy(i).start()
    seen[me] = packed_ref[...]
    for i in range(1, owners):
        copy(i).wait()
    holder = lax.broadcasted_iota(jnp.int32, packed_ref.shape, 0)
    for o in range(owners):
        token = seen[o]
        count, word = token & 3, token >> 2
        row = word - me * vocab
        ours = (count > 0) & (row >= 0) & (row < vocab)
        key = (row * all_docs + (holder + o * doc_rows)) * 4 + count
        key_ref[o * doc_rows:(o + 1) * doc_rows, :] = jnp.where(ours, key, vocab * all_docs * 4)


def share_tokens(packed, vocab):
    owners, (doc_rows, length) = lax.axis_size("docs"), packed.shape
    vmem = pl.BlockSpec(memory_space=pltpu.VMEM)
    return pl.pallas_call(
        functools.partial(share_kernel, owners, vocab),
        out_shape=jax.ShapeDtypeStruct((owners * doc_rows, length), jnp.int32),
        in_specs=[vmem],
        out_specs=vmem,
        scratch_shapes=[
            pltpu.VMEM((owners, doc_rows, length), jnp.int32),
            pltpu.SemaphoreType.DMA((owners,)),
            pltpu.SemaphoreType.DMA((owners,)),
        ],
        compiler_params=pltpu.CompilerParams(collective_id=1, has_side_effects=True),
    )(packed)


def make_windows(row_ref, table):
    lines = row_ref.shape[0] - 8
    here, after = row_ref[:lines, :], row_ref[1:lines + 1, :]
    lane = lax.broadcasted_iota(jnp.int32, here.shape, 1)
    table[:lines, :] = here
    for k in range(1, PIECE // STEP):
        back = PIECE - k * STEP
        table[k * lines:(k + 1) * lines, :] = jnp.where(
            lane < back, pltpu.roll(here, back, 1), pltpu.roll(after, back, 1)
        )


def window_rows(table, start):
    lines = table.shape[0] * STEP // PIECE
    place = lax.rem(start, PIECE) // STEP * lines + start // PIECE
    return table[pl.ds(place, 1), :]


def gather_kernel(bound_ref, row_ref, beta_ref, out_ref, table, held, sems):
    depth, height, cols = held.shape
    steps = beta_ref.shape[0] // height
    parts = height // SUB

    def copy(s):
        slot = lax.rem(s, depth)
        rows = pl.ds(pl.multiple_of(s * height, height), height)
        return pltpu.make_async_copy(beta_ref.at[rows], held.at[slot], sems.at[slot])

    for s in range(depth):
        copy(s).start()
    make_windows(row_ref, table)
    out_ref[...] = jnp.zeros_like(out_ref)
    lane_row = lax.broadcasted_iota(jnp.int32, (SUB, PIECE), 0)

    def fetch(s, part, start):
        base = (s * parts + part) * SUB
        hit = jnp.where(lane_row == window_rows(table, start) - base, 1.0, 0.0).astype(jnp.bfloat16)
        rows = tn(hit, held[lax.rem(s, depth), part * SUB:(part + 1) * SUB, :])
        place = pl.ds(pl.multiple_of(start, STEP), PIECE)
        out_ref[place, :] = (out_ref[place, :].astype(jnp.float32) + rows).astype(out_ref.dtype)

    def step(s, carry):
        copy(s).wait()
        firsts = []
        for part in range(parts):
            firsts.append(bound_ref[s * parts + part] // STEP * STEP)
            fetch(s, part, firsts[-1])
        for part in range(parts):
            end = bound_ref[s * parts + part + 1]

            def more(i, carry, part=part):
                fetch(s, part, firsts[part] + i * PIECE)
                return carry

            lax.fori_loop(1, (end - firsts[part] + PIECE - 1) // PIECE, more, 0)

        @pl.when(s + depth < steps)
        def _():
            copy(s + depth).start()

        return carry

    lax.fori_loop(0, steps, step, 0)


def gather_rows(log_beta, rows, bounds):
    (total, cols), slots = log_beta.shape, (rows.shape[0] - 8) * PIECE
    height = 1024
    depth = min(8, total // height)
    return pl.pallas_call(
        gather_kernel,
        out_shape=jax.ShapeDtypeStruct((slots + PIECE, cols), log_beta.dtype),
        in_specs=[
            pl.BlockSpec(memory_space=pltpu.SMEM),
            pl.BlockSpec(memory_space=pltpu.VMEM),
            pl.BlockSpec(memory_space=pl.ANY),
        ],
        out_specs=pl.BlockSpec(memory_space=pltpu.VMEM),
        scratch_shapes=[
            pltpu.VMEM((slots // STEP, PIECE), jnp.int32),
            pltpu.VMEM((depth, height, cols), log_beta.dtype),
            pltpu.SemaphoreType.DMA((depth,)),
        ],
        compiler_params=pltpu.CompilerParams(vmem_limit_bytes=GATHER_LIMIT),
    )(bounds, rows, log_beta)


def nt(a, b):
    return lax.dot_general(a, b, (((1,), (1,)), ((), ())), preferred_element_type=jnp.float32)


def tn(a, b):
    return lax.dot_general(a, b, (((0,), (0,)), ((), ())), preferred_element_type=jnp.float32)


def nn(a, b):
    return jnp.dot(a, b, preferred_element_type=jnp.float32)


def split(x):
    high = x.astype(jnp.bfloat16)
    return high, (x - high.astype(jnp.float32)).astype(jnp.bfloat16)


def digamma(x):
    top, bottom = jnp.ones_like(x), x
    for i in range(1, 8):
        top = top * (x + i) + bottom
        bottom = bottom * (x + i)
    y = x + 8.0
    inv = 1.0 / y
    sq = inv * inv
    series = sq * (1.0 / 12 - sq * (1.0 / 120 - sq * (1.0 / 252)))
    return jnp.log(y) - 0.5 * inv - series - top / bottom


def sweep_kernel(
    owners, parts, found_ref, doc_ref, count_ref, gamma_ref, prior_ref,
    gamma_out, high, low,
    weights, theta_two, placed, sums, theta_all, theta_mine, sums_in, tops, norms, scale,
    theta_send, theta_recv, sums_send, sums_recv, top_send, top_recv, norm_send, norm_recv,
):
    me, part = lax.axis_index("docs"), lax.axis_index("topics")
    lines = doc_ref.shape[0]
    tokens, cols = lines * LANES, high.shape[1]
    doc_rows = gamma_ref.shape[0]
    docs = owners * doc_rows
    half = cols // HALVES
    block = DEEP // LANES
    blocks = tokens // DEEP
    others = sorted(range(1, owners), key=lambda i: abs(2 * i - owners))

    def owner(i):
        return lax.rem(me + i, owners)

    def fellow(i):
        return lax.rem(part + i, parts)

    barrier = pltpu.get_barrier_semaphore()
    for i in others:
        pl.semaphore_signal(barrier, inc=1, device_id=(owner(i), part), device_id_type=MESH)
    for i in range(1, parts):
        pl.semaphore_signal(barrier, inc=1, device_id=(me, fellow(i)), device_id_type=MESH)

    mine = pl.ds(pl.multiple_of(me * doc_rows, doc_rows), doc_rows)

    def side(h):
        return slice(h * half, (h + 1) * half)

    def theta_copy(h, i):
        return pltpu.make_async_remote_copy(
            src_ref=theta_mine.at[h], dst_ref=theta_all.at[h, mine],
            send_sem=theta_send.at[h, i], recv_sem=theta_recv.at[h, i],
            device_id=(owner(i), part), device_id_type=MESH,
        )

    def sums_copy(h, i):
        theirs = pl.ds(pl.multiple_of(owner(i) * doc_rows, doc_rows), doc_rows)
        return pltpu.make_async_remote_copy(
            src_ref=sums.at[h, theirs], dst_ref=sums_in.at[h, i],
            send_sem=sums_send.at[h, i], recv_sem=sums_recv.at[h, i],
            device_id=(owner(i), part), device_id_type=MESH,
        )

    def top_copy(i):
        return pltpu.make_async_remote_copy(
            src_ref=tops.at[0], dst_ref=tops.at[i], send_sem=top_send.at[i], recv_sem=top_recv.at[i],
            device_id=(me, fellow(i)), device_id_type=MESH,
        )

    def norm_copy(i, turn, q):
        piece = pl.ds(pl.multiple_of(q * block, block), block)
        return pltpu.make_async_remote_copy(
            src_ref=norms.at[turn, 0, piece], dst_ref=norms.at[turn, i, piece],
            send_sem=norm_send.at[turn, i, q], recv_sem=norm_recv.at[turn, i, q],
            device_id=(me, fellow(i)), device_id_type=MESH,
        )

    def send_theta(h, gamma):
        theta_mine[h] = jnp.exp(digamma(gamma))
        for i in others:
            theta_copy(h, i).start()
        theta_all[h, mine, :] = theta_mine[h]

    pl.semaphore_wait(barrier, owners + parts - 2)
    for h in range(HALVES):
        send_theta(h, gamma_ref[:, side(h)])

    pick = jnp.where(lax.broadcasted_iota(jnp.int32, (16, PIECE), 1) == 0, 1.0, 0.0).astype(jnp.bfloat16)

    def make_mass(c, carry):
        rows = pl.ds(pl.multiple_of(c * LANES, LANES), LANES)
        x = found_ref[rows, :].astype(jnp.float32)
        top = jnp.max(x, axis=1, keepdims=True)
        high[rows, :], low[rows, :] = split(jnp.exp(x - top))
        wide = jnp.broadcast_to(top, (LANES, PIECE)).astype(jnp.bfloat16)
        tops[0, pl.ds(c, 1), :] = nt(pick, wide)[:1]
        return carry

    lax.fori_loop(0, lines, make_mass, 0, unroll=4)
    for i in range(1, parts):
        top_copy(i).start()

    lane_doc = lax.broadcasted_iota(jnp.int32, (docs, LANES), 0)

    def deep_rows(q):
        return pl.ds(pl.multiple_of(q * DEEP, DEEP), DEEP)

    def block_lines(q):
        return pl.ds(pl.multiple_of(q * block, block), block)

    def products(turn):
        def step(q, carry):
            both = nt(theta_two[...], high[deep_rows(q), :])
            less = nt(theta_two[:docs, :], low[deep_rows(q), :])
            total = both[:docs] + both[docs:] + less
            for j in range(block):
                line = pl.ds(q * block + j, 1)
                chosen = jnp.where(lane_doc == doc_ref[line, :], total[:, j * LANES:(j + 1) * LANES], 0.0)
                norms[turn, 0, line, :] = jnp.sum(chosen, axis=0, keepdims=True)
            for i in range(1, parts):
                norm_copy(i, turn, q).start()
            return carry

        lax.fori_loop(0, blocks, step, 0)

    def new_weights(turn, q):
        piece = block_lines(q)
        for i in range(1, parts):
            norm_copy(i, turn, q).wait()
        norm = scale[0, piece, :] * norms[turn, 0, piece, :]
        for i in range(1, parts):
            norm = norm + scale[i, piece, :] * norms[turn, i, piece, :]
        weights[piece, :] = count_ref[piece, :] * scale[0, piece, :] / norm

    def add_sums(h, q):
        both = nn(placed[q], high[deep_rows(q), side(h)])
        less = nn(placed[q, :docs], low[deep_rows(q), side(h)])
        sums[h] += both[:docs] + both[docs:] + less

    def first_sums(turn):
        def step(q, carry):
            new_weights(turn, q)
            for j in range(block):
                line = pl.ds(q * block + j, 1)
                h, l = split(jnp.where(lane_doc == doc_ref[line, :], weights[line, :], 0.0))
                placed[q, :docs, j * LANES:(j + 1) * LANES] = h
                placed[q, docs:, j * LANES:(j + 1) * LANES] = l
            add_sums(0, q)
            return carry

        lax.fori_loop(0, blocks, step, 0)

    def later_sums(h):
        def step(q, carry):
            add_sums(h, q)
            return carry

        lax.fori_loop(0, blocks, step, 0)

    def spread(c, carry):
        rows = pl.ds(pl.multiple_of(c * LANES, LANES), LANES)
        wh, wl = split(jnp.where(lane_doc == doc_ref[pl.ds(c, 1), :], weights[pl.ds(c, 1), :], 0.0))
        theta = tn(jnp.concatenate([wh, wh], axis=0), theta_two[...]) + tn(wl, theta_two[:docs, :])
        mass = high[rows, :].astype(jnp.float32) + low[rows, :].astype(jnp.float32)
        high[rows, :], low[rows, :] = split(mass * theta)
        return carry

    for sweep in range(ITERS + 1):
        turn = sweep % 2
        for h in range(HALVES):
            for i in others:
                theta_copy(h, i).wait()
            theta_two[:docs, side(h)], theta_two[docs:, side(h)] = split(theta_all[h])
        products(turn)
        if sweep == 0:
            for i in range(1, parts):
                top_copy(i).wait()
            peak = tops[0]
            for i in range(1, parts):
                peak = jnp.maximum(peak, tops[i])
            for i in range(parts):
                scale[i] = jnp.exp(tops[i] - peak)
        if sweep < ITERS:
            sums[...] = jnp.zeros_like(sums)
            first_sums(turn)
            for i in others:
                sums_copy(0, i).start()
            for h in range(1, HALVES):
                later_sums(h)
                for i in others:
                    sums_copy(h, i).start()
            for h in range(HALVES):
                total = sums[h, mine, :]
                for i in others:
                    sums_copy(h, i).wait_recv()
                    total = total + sums_in[h, i]
                renewed = prior_ref[:, side(h)] + theta_mine[h] * total
                if sweep == ITERS - 1:
                    gamma_out[:, side(h)] = renewed
                send_theta(h, renewed)
            for h in range(HALVES):
                for i in others:
                    sums_copy(h, i).wait_send()
        else:
            def finish(q, carry):
                new_weights(turn, q)
                return lax.fori_loop(0, block, lambda j, c: spread(q * block + j, c), carry, unroll=4)

            lax.fori_loop(0, blocks, finish, 0)
    high[tokens:, :] = jnp.zeros((PIECE, cols), high.dtype)
    low[tokens:, :] = jnp.zeros((PIECE, cols), low.dtype)


def run_sweeps(found, docs, count, gamma_init, topic_prior):
    owners, parts = lax.axis_size("docs"), lax.axis_size("topics")
    (padded, cols), doc_rows, tokens = found.shape, gamma_init.shape[0], docs.shape[0]
    all_docs, lines, half = owners * doc_rows, tokens // LANES, cols // HALVES
    blocks = tokens // DEEP
    vmem = pl.BlockSpec(memory_space=pltpu.VMEM)
    f32, bf16, dma = jnp.float32, jnp.bfloat16, pltpu.SemaphoreType.DMA
    return pl.pallas_call(
        functools.partial(sweep_kernel, owners, parts),
        out_shape=(
            jax.ShapeDtypeStruct((doc_rows, cols), f32),
            jax.ShapeDtypeStruct((padded, cols), bf16),
            jax.ShapeDtypeStruct((padded, cols), bf16),
        ),
        in_specs=[vmem] * 5,
        out_specs=(vmem,) * 3,
        scratch_shapes=[
            pltpu.VMEM((lines, LANES), f32),
            pltpu.VMEM((2 * all_docs, cols), bf16),
            pltpu.VMEM((blocks, 2 * all_docs, DEEP), bf16),
            pltpu.VMEM((HALVES, all_docs, half), f32),
            pltpu.VMEM((HALVES, all_docs, half), f32),
            pltpu.VMEM((HALVES, doc_rows, half), f32),
            pltpu.VMEM((HALVES, owners, doc_rows, half), f32),
            pltpu.VMEM((parts, lines, LANES), f32),
            pltpu.VMEM((2, parts, lines, LANES), f32),
            pltpu.VMEM((parts, lines, LANES), f32),
            dma((HALVES, owners)), dma((HALVES, owners)), dma((HALVES, owners)), dma((HALVES, owners)),
            dma((parts,)), dma((parts,)), dma((2, parts, blocks)), dma((2, parts, blocks)),
        ],
        compiler_params=pltpu.CompilerParams(
            collective_id=0, has_side_effects=True,
            vmem_limit_bytes=SWEEP_LIMIT + 4 * all_docs * tokens,
        ),
    )(found, docs.reshape(lines, LANES), count.reshape(lines, LANES), gamma_init, topic_prior[None, :])


def stats_kernel(bound_ref, row_ref, high_ref, low_ref, out_ref, table, held, sems):
    depth, height, cols = held.shape
    steps = out_ref.shape[0] // height
    parts = height // SUB
    make_windows(row_ref, table)
    lane_row = lax.broadcasted_iota(jnp.int32, (SUB, PIECE), 0)

    def copy(s):
        slot = lax.rem(s, depth)
        rows = pl.ds(pl.multiple_of(s * height, height), height)
        return pltpu.make_async_copy(held.at[slot], out_ref.at[rows], sems.at[slot])

    def spread(s, part, start):
        base = (s * parts + part) * SUB
        hit = jnp.where(lane_row == window_rows(table, start) - base, 1.0, 0.0).astype(jnp.bfloat16)
        place = pl.ds(pl.multiple_of(start, STEP), PIECE)
        both = jnp.concatenate([high_ref[place, :], low_ref[place, :]], axis=0)
        return nn(jnp.concatenate([hit, hit], axis=1), both)

    def step(s, carry):
        slot = lax.rem(s, depth)

        @pl.when(s >= depth)
        def _():
            copy(s - depth).wait()

        firsts = []
        for part in range(parts):
            firsts.append(bound_ref[s * parts + part] // STEP * STEP)
            held[slot, part * SUB:(part + 1) * SUB, :] = spread(s, part, firsts[-1])
        for part in range(parts):
            end = bound_ref[s * parts + part + 1]

            def more(i, carry, part=part):
                held[slot, part * SUB:(part + 1) * SUB, :] += spread(s, part, firsts[part] + i * PIECE)
                return carry

            lax.fori_loop(1, (end - firsts[part] + PIECE - 1) // PIECE, more, 0)
        copy(s).start()
        return carry

    lax.fori_loop(0, steps, step, 0)
    for s in range(steps - depth, steps):
        copy(s).wait()


def write_stats(bounds, rows, high, low, total):
    padded, cols = high.shape
    vmem = pl.BlockSpec(memory_space=pltpu.VMEM)
    height = 512
    depth = min(8, total // height)
    return pl.pallas_call(
        stats_kernel,
        out_shape=jax.ShapeDtypeStruct((total, cols), jnp.float32),
        in_specs=[pl.BlockSpec(memory_space=pltpu.SMEM), vmem, vmem, vmem],
        out_specs=pl.BlockSpec(memory_space=pl.ANY),
        scratch_shapes=[
            pltpu.VMEM(((padded - PIECE) // STEP, PIECE), jnp.int32),
            pltpu.VMEM((depth, height, cols), jnp.float32),
            pltpu.SemaphoreType.DMA((depth,)),
        ],
        compiler_params=pltpu.CompilerParams(vmem_limit_bytes=STATS_LIMIT),
    )(bounds, rows, high, low)


def per_device(log_beta, gamma_init, topic_prior, word_block, word_row, counts):
    doc_rows, length = counts.shape
    vocab = log_beta.shape[0]
    all_docs = lax.axis_size("docs") * doc_rows
    slots = 2 * doc_rows * length

    packed = (word_block[:, :, 0] * vocab + word_row) * 4 + counts
    key = lax.sort(share_tokens(packed, vocab).reshape(-1))[:slots]
    blank = vocab * all_docs * 4
    rows = jnp.minimum(key // (4 * all_docs), vocab - 1)
    docs = (key // 4) % all_docs
    count = jnp.where(key < blank, key % 4, 0).astype(jnp.float32)
    limits = jnp.arange(0, vocab + 1, SUB, dtype=jnp.int32) * (all_docs * 4)
    bounds = jnp.sum(key[None, :] < limits[:, None], axis=1, dtype=jnp.int32)
    lines = jnp.pad(rows.reshape(slots // PIECE, PIECE), ((0, 8), (0, 0)), constant_values=-1)

    found = gather_rows(log_beta, lines, bounds)
    doc_gamma, high, low = run_sweeps(found, docs, count, gamma_init, topic_prior)
    sstats = write_stats(bounds, lines, high, low, vocab)
    return (doc_gamma, sstats)


def solution(mesh):
    in_specs = (
        P("docs", "topics"),
        P("docs", "topics"),
        P("topics"),
        P("docs", None, None),
        P("docs", None),
        P("docs", None),
    )
    out_specs = (P("docs", "topics"), P("docs", "topics"))
    return jax.shard_map(
        per_device, mesh=mesh, in_specs=in_specs, out_specs=out_specs, check_vma=False
    )
```

```python
import functools

import jax
import jax.numpy as jnp
from jax import lax
from jax.experimental import pallas as pl
from jax.experimental.pallas import tpu as pltpu
from jax.sharding import PartitionSpec as P

ITERS = 3
MESH = pl.DeviceIdType.MESH
LANES = 256
DEEP = 2048
PIECE = 128
SUB = 256
STEP = 16
HALVES = 2
GATHER_LIMIT = 16 * 1024 * 1024
SWEEP_LIMIT = 12 * 1024 * 1024
STATS_LIMIT = 16 * 1024 * 1024


def share_kernel(owners, vocab, packed_ref, key_ref, seen, send, recv):
    me, part = lax.axis_index("docs"), lax.axis_index("topics")
    doc_rows = packed_ref.shape[0]
    all_docs = owners * doc_rows

    def owner(i):
        return lax.rem(me + i, owners)

    barrier = pltpu.get_barrier_semaphore()
    for i in range(1, owners):
        pl.semaphore_signal(barrier, inc=1, device_id=(owner(i), part), device_id_type=MESH)
    pl.semaphore_wait(barrier, owners - 1)

    def copy(i):
        return pltpu.make_async_remote_copy(
            src_ref=packed_ref, dst_ref=seen.at[me], send_sem=send.at[i], recv_sem=recv.at[i],
            device_id=(owner(i), part), device_id_type=MESH,
        )

    for i in range(1, owners):
        copy(i).start()
    seen[me] = packed_ref[...]
    for i in range(1, owners):
        copy(i).wait()
    holder = lax.broadcasted_iota(jnp.int32, packed_ref.shape, 0)
    for o in range(owners):
        token = seen[o]
        count, word = token & 3, token >> 2
        row = word - me * vocab
        ours = (count > 0) & (row >= 0) & (row < vocab)
        key = (row * all_docs + (holder + o * doc_rows)) * 4 + count
        key_ref[o * doc_rows:(o + 1) * doc_rows, :] = jnp.where(ours, key, vocab * all_docs * 4)


def share_tokens(packed, vocab):
    owners, (doc_rows, length) = lax.axis_size("docs"), packed.shape
    vmem = pl.BlockSpec(memory_space=pltpu.VMEM)
    return pl.pallas_call(
        functools.partial(share_kernel, owners, vocab),
        out_shape=jax.ShapeDtypeStruct((owners * doc_rows, length), jnp.int32),
        in_specs=[vmem],
        out_specs=vmem,
        scratch_shapes=[
            pltpu.VMEM((owners, doc_rows, length), jnp.int32),
            pltpu.SemaphoreType.DMA((owners,)),
            pltpu.SemaphoreType.DMA((owners,)),
        ],
        compiler_params=pltpu.CompilerParams(collective_id=1, has_side_effects=True),
    )(packed)


def make_windows(row_ref, table):
    lines = row_ref.shape[0] - 8
    here, after = row_ref[:lines, :], row_ref[1:lines + 1, :]
    lane = lax.broadcasted_iota(jnp.int32, here.shape, 1)
    table[:lines, :] = here
    for k in range(1, PIECE // STEP):
        back = PIECE - k * STEP
        table[k * lines:(k + 1) * lines, :] = jnp.where(
            lane < back, pltpu.roll(here, back, 1), pltpu.roll(after, back, 1)
        )


def window_rows(table, start):
    lines = table.shape[0] * STEP // PIECE
    place = lax.rem(start, PIECE) // STEP * lines + start // PIECE
    return table[pl.ds(place, 1), :]


def gather_kernel(bound_ref, row_ref, beta_ref, out_ref, table, held, sems):
    depth, height, cols = held.shape
    steps = beta_ref.shape[0] // height
    parts = height // SUB

    def copy(s):
        slot = lax.rem(s, depth)
        rows = pl.ds(pl.multiple_of(s * height, height), height)
        return pltpu.make_async_copy(beta_ref.at[rows], held.at[slot], sems.at[slot])

    for s in range(depth):
        copy(s).start()
    make_windows(row_ref, table)
    out_ref[...] = jnp.zeros_like(out_ref)
    lane_row = lax.broadcasted_iota(jnp.int32, (SUB, PIECE), 0)

    def fetch(s, part, start):
        base = (s * parts + part) * SUB
        hit = jnp.where(lane_row == window_rows(table, start) - base, 1.0, 0.0).astype(jnp.bfloat16)
        rows = tn(hit, held[lax.rem(s, depth), part * SUB:(part + 1) * SUB, :])
        place = pl.ds(pl.multiple_of(start, STEP), PIECE)
        out_ref[place, :] = (out_ref[place, :].astype(jnp.float32) + rows).astype(out_ref.dtype)

    def step(s, carry):
        copy(s).wait()
        firsts = []
        for part in range(parts):
            firsts.append(bound_ref[s * parts + part] // STEP * STEP)
            fetch(s, part, firsts[-1])
        for part in range(parts):
            end = bound_ref[s * parts + part + 1]

            def more(i, carry, part=part):
                fetch(s, part, firsts[part] + i * PIECE)
                return carry

            lax.fori_loop(1, (end - firsts[part] + PIECE - 1) // PIECE, more, 0)

        @pl.when(s + depth < steps)
        def _():
            copy(s + depth).start()

        return carry

    lax.fori_loop(0, steps, step, 0)


def gather_rows(log_beta, rows, bounds):
    (total, cols), slots = log_beta.shape, (rows.shape[0] - 8) * PIECE
    height = 2048
    depth = min(4, total // height)
    return pl.pallas_call(
        gather_kernel,
        out_shape=jax.ShapeDtypeStruct((slots + PIECE, cols), log_beta.dtype),
        in_specs=[
            pl.BlockSpec(memory_space=pltpu.SMEM),
            pl.BlockSpec(memory_space=pltpu.VMEM),
            pl.BlockSpec(memory_space=pl.ANY),
        ],
        out_specs=pl.BlockSpec(memory_space=pltpu.VMEM),
        scratch_shapes=[
            pltpu.VMEM((slots // STEP, PIECE), jnp.int32),
            pltpu.VMEM((depth, height, cols), log_beta.dtype),
            pltpu.SemaphoreType.DMA((depth,)),
        ],
        compiler_params=pltpu.CompilerParams(vmem_limit_bytes=GATHER_LIMIT),
    )(bounds, rows, log_beta)


def nt(a, b):
    return lax.dot_general(a, b, (((1,), (1,)), ((), ())), preferred_element_type=jnp.float32)


def tn(a, b):
    return lax.dot_general(a, b, (((0,), (0,)), ((), ())), preferred_element_type=jnp.float32)


def nn(a, b):
    return jnp.dot(a, b, preferred_element_type=jnp.float32)


def split(x):
    high = x.astype(jnp.bfloat16)
    return high, (x - high.astype(jnp.float32)).astype(jnp.bfloat16)


def digamma(x):
    top, bottom = jnp.ones_like(x), x
    for i in range(1, 8):
        top = top * (x + i) + bottom
        bottom = bottom * (x + i)
    y = x + 8.0
    inv = 1.0 / y
    sq = inv * inv
    series = sq * (1.0 / 12 - sq * (1.0 / 120 - sq * (1.0 / 252)))
    return jnp.log(y) - 0.5 * inv - series - top / bottom


def sweep_kernel(
    owners, parts, found_ref, doc_ref, count_ref, gamma_ref, prior_ref,
    gamma_out, high, low,
    weights, theta_two, placed, sums, theta_all, theta_mine, sums_in, tops, norms, scale,
    theta_send, theta_recv, sums_send, sums_recv, top_send, top_recv, norm_send, norm_recv,
):
    me, part = lax.axis_index("docs"), lax.axis_index("topics")
    lines = doc_ref.shape[0]
    tokens, cols = lines * LANES, high.shape[1]
    doc_rows = gamma_ref.shape[0]
    docs = owners * doc_rows
    half = cols // HALVES
    block = DEEP // LANES
    blocks = tokens // DEEP
    others = sorted(range(1, owners), key=lambda i: abs(2 * i - owners))

    def owner(i):
        return lax.rem(me + i, owners)

    def fellow(i):
        return lax.rem(part + i, parts)

    barrier = pltpu.get_barrier_semaphore()
    for i in others:
        pl.semaphore_signal(barrier, inc=1, device_id=(owner(i), part), device_id_type=MESH)
    for i in range(1, parts):
        pl.semaphore_signal(barrier, inc=1, device_id=(me, fellow(i)), device_id_type=MESH)

    mine = pl.ds(pl.multiple_of(me * doc_rows, doc_rows), doc_rows)

    def side(h):
        return slice(h * half, (h + 1) * half)

    def theta_copy(h, i):
        return pltpu.make_async_remote_copy(
            src_ref=theta_mine.at[h], dst_ref=theta_all.at[h, mine],
            send_sem=theta_send.at[h, i], recv_sem=theta_recv.at[h, i],
            device_id=(owner(i), part), device_id_type=MESH,
        )

    def sums_copy(h, i):
        theirs = pl.ds(pl.multiple_of(owner(i) * doc_rows, doc_rows), doc_rows)
        return pltpu.make_async_remote_copy(
            src_ref=sums.at[h, theirs], dst_ref=sums_in.at[h, i],
            send_sem=sums_send.at[h, i], recv_sem=sums_recv.at[h, i],
            device_id=(owner(i), part), device_id_type=MESH,
        )

    def top_copy(i):
        return pltpu.make_async_remote_copy(
            src_ref=tops.at[0], dst_ref=tops.at[i], send_sem=top_send.at[i], recv_sem=top_recv.at[i],
            device_id=(me, fellow(i)), device_id_type=MESH,
        )

    def norm_copy(i, turn, q):
        piece = pl.ds(pl.multiple_of(q * block, block), block)
        return pltpu.make_async_remote_copy(
            src_ref=norms.at[turn, 0, piece], dst_ref=norms.at[turn, i, piece],
            send_sem=norm_send.at[turn, i, q], recv_sem=norm_recv.at[turn, i, q],
            device_id=(me, fellow(i)), device_id_type=MESH,
        )

    def send_theta(h, gamma):
        theta_mine[h] = jnp.exp(digamma(gamma))
        for i in others:
            theta_copy(h, i).start()
        theta_all[h, mine, :] = theta_mine[h]

    pl.semaphore_wait(barrier, owners + parts - 2)
    for h in range(HALVES):
        send_theta(h, gamma_ref[:, side(h)])

    pick = jnp.where(lax.broadcasted_iota(jnp.int32, (16, PIECE), 1) == 0, 1.0, 0.0).astype(jnp.bfloat16)

    def make_mass(c, carry):
        rows = pl.ds(pl.multiple_of(c * LANES, LANES), LANES)
        x = found_ref[rows, :].astype(jnp.float32)
        top = jnp.max(x, axis=1, keepdims=True)
        high[rows, :], low[rows, :] = split(jnp.exp(x - top))
        wide = jnp.broadcast_to(top, (LANES, PIECE)).astype(jnp.bfloat16)
        tops[0, pl.ds(c, 1), :] = nt(pick, wide)[:1]
        return carry

    lax.fori_loop(0, lines, make_mass, 0, unroll=4)
    for i in range(1, parts):
        top_copy(i).start()

    lane_doc = lax.broadcasted_iota(jnp.int32, (docs, LANES), 0)

    def deep_rows(q):
        return pl.ds(pl.multiple_of(q * DEEP, DEEP), DEEP)

    def block_lines(q):
        return pl.ds(pl.multiple_of(q * block, block), block)

    def products(turn):
        def step(q, carry):
            both = nt(theta_two[...], high[deep_rows(q), :])
            less = nt(theta_two[:docs, :], low[deep_rows(q), :])
            total = both[:docs] + both[docs:] + less
            for j in range(block):
                line = pl.ds(q * block + j, 1)
                chosen = jnp.where(lane_doc == doc_ref[line, :], total[:, j * LANES:(j + 1) * LANES], 0.0)
                norms[turn, 0, line, :] = jnp.sum(chosen, axis=0, keepdims=True)
            for i in range(1, parts):
                norm_copy(i, turn, q).start()
            return carry

        lax.fori_loop(0, blocks, step, 0)

    def new_weights(turn, q):
        piece = block_lines(q)
        for i in range(1, parts):
            norm_copy(i, turn, q).wait()
        norm = scale[0, piece, :] * norms[turn, 0, piece, :]
        for i in range(1, parts):
            norm = norm + scale[i, piece, :] * norms[turn, i, piece, :]
        weights[piece, :] = count_ref[piece, :] * scale[0, piece, :] / norm

    def add_sums(h, q):
        both = nn(placed[q], high[deep_rows(q), side(h)])
        less = nn(placed[q, :docs], low[deep_rows(q), side(h)])
        sums[h] += both[:docs] + both[docs:] + less

    def first_sums(turn):
        def step(q, carry):
            new_weights(turn, q)
            for j in range(block):
                line = pl.ds(q * block + j, 1)
                h, l = split(jnp.where(lane_doc == doc_ref[line, :], weights[line, :], 0.0))
                placed[q, :docs, j * LANES:(j + 1) * LANES] = h
                placed[q, docs:, j * LANES:(j + 1) * LANES] = l
            add_sums(0, q)
            return carry

        lax.fori_loop(0, blocks, step, 0)

    def later_sums(h):
        def step(q, carry):
            add_sums(h, q)
            return carry

        lax.fori_loop(0, blocks, step, 0)

    def spread(c, carry):
        rows = pl.ds(pl.multiple_of(c * LANES, LANES), LANES)
        wh, wl = split(jnp.where(lane_doc == doc_ref[pl.ds(c, 1), :], weights[pl.ds(c, 1), :], 0.0))
        theta = tn(jnp.concatenate([wh, wh], axis=0), theta_two[...]) + tn(wl, theta_two[:docs, :])
        mass = high[rows, :].astype(jnp.float32) + low[rows, :].astype(jnp.float32)
        high[rows, :], low[rows, :] = split(mass * theta)
        return carry

    for sweep in range(ITERS + 1):
        turn = sweep % 2
        for h in range(HALVES):
            for i in others:
                theta_copy(h, i).wait()
            theta_two[:docs, side(h)], theta_two[docs:, side(h)] = split(theta_all[h])
        products(turn)
        if sweep == 0:
            for i in range(1, parts):
                top_copy(i).wait()
            peak = tops[0]
            for i in range(1, parts):
                peak = jnp.maximum(peak, tops[i])
            for i in range(parts):
                scale[i] = jnp.exp(tops[i] - peak)
        if sweep < ITERS:
            sums[...] = jnp.zeros_like(sums)
            first_sums(turn)
            for i in others:
                sums_copy(0, i).start()
            for h in range(1, HALVES):
                later_sums(h)
                for i in others:
                    sums_copy(h, i).start()
            for h in range(HALVES):
                total = sums[h, mine, :]
                for i in others:
                    sums_copy(h, i).wait_recv()
                    total = total + sums_in[h, i]
                renewed = prior_ref[:, side(h)] + theta_mine[h] * total
                if sweep == ITERS - 1:
                    gamma_out[:, side(h)] = renewed
                send_theta(h, renewed)
            for h in range(HALVES):
                for i in others:
                    sums_copy(h, i).wait_send()
        else:
            def finish(q, carry):
                new_weights(turn, q)
                return lax.fori_loop(0, block, lambda j, c: spread(q * block + j, c), carry, unroll=4)

            lax.fori_loop(0, blocks, finish, 0)
    high[tokens:, :] = jnp.zeros((PIECE, cols), high.dtype)
    low[tokens:, :] = jnp.zeros((PIECE, cols), low.dtype)


def run_sweeps(found, docs, count, gamma_init, topic_prior):
    owners, parts = lax.axis_size("docs"), lax.axis_size("topics")
    (padded, cols), doc_rows, tokens = found.shape, gamma_init.shape[0], docs.shape[0]
    all_docs, lines, half = owners * doc_rows, tokens // LANES, cols // HALVES
    blocks = tokens // DEEP
    vmem = pl.BlockSpec(memory_space=pltpu.VMEM)
    f32, bf16, dma = jnp.float32, jnp.bfloat16, pltpu.SemaphoreType.DMA
    return pl.pallas_call(
        functools.partial(sweep_kernel, owners, parts),
        out_shape=(
            jax.ShapeDtypeStruct((doc_rows, cols), f32),
            jax.ShapeDtypeStruct((padded, cols), bf16),
            jax.ShapeDtypeStruct((padded, cols), bf16),
        ),
        in_specs=[vmem] * 5,
        out_specs=(vmem,) * 3,
        scratch_shapes=[
            pltpu.VMEM((lines, LANES), f32),
            pltpu.VMEM((2 * all_docs, cols), bf16),
            pltpu.VMEM((blocks, 2 * all_docs, DEEP), bf16),
            pltpu.VMEM((HALVES, all_docs, half), f32),
            pltpu.VMEM((HALVES, all_docs, half), f32),
            pltpu.VMEM((HALVES, doc_rows, half), f32),
            pltpu.VMEM((HALVES, owners, doc_rows, half), f32),
            pltpu.VMEM((parts, lines, LANES), f32),
            pltpu.VMEM((2, parts, lines, LANES), f32),
            pltpu.VMEM((parts, lines, LANES), f32),
            dma((HALVES, owners)), dma((HALVES, owners)), dma((HALVES, owners)), dma((HALVES, owners)),
            dma((parts,)), dma((parts,)), dma((2, parts, blocks)), dma((2, parts, blocks)),
        ],
        compiler_params=pltpu.CompilerParams(
            collective_id=0, has_side_effects=True,
            vmem_limit_bytes=SWEEP_LIMIT + 4 * all_docs * tokens,
        ),
    )(found, docs.reshape(lines, LANES), count.reshape(lines, LANES), gamma_init, topic_prior[None, :])


def stats_kernel(bound_ref, row_ref, high_ref, low_ref, out_ref, table, held, sems):
    depth, height, cols = held.shape
    steps = out_ref.shape[0] // height
    parts = height // SUB
    make_windows(row_ref, table)
    lane_row = lax.broadcasted_iota(jnp.int32, (SUB, PIECE), 0)

    def copy(s):
        slot = lax.rem(s, depth)
        rows = pl.ds(pl.multiple_of(s * height, height), height)
        return pltpu.make_async_copy(held.at[slot], out_ref.at[rows], sems.at[slot])

    def spread(s, part, start):
        base = (s * parts + part) * SUB
        hit = jnp.where(lane_row == window_rows(table, start) - base, 1.0, 0.0).astype(jnp.bfloat16)
        place = pl.ds(pl.multiple_of(start, STEP), PIECE)
        both = jnp.concatenate([high_ref[place, :], low_ref[place, :]], axis=0)
        return nn(jnp.concatenate([hit, hit], axis=1), both)

    def step(s, carry):
        slot = lax.rem(s, depth)

        @pl.when(s >= depth)
        def _():
            copy(s - depth).wait()

        firsts = []
        for part in range(parts):
            firsts.append(bound_ref[s * parts + part] // STEP * STEP)
            held[slot, part * SUB:(part + 1) * SUB, :] = spread(s, part, firsts[-1])
        for part in range(parts):
            end = bound_ref[s * parts + part + 1]

            def more(i, carry, part=part):
                held[slot, part * SUB:(part + 1) * SUB, :] += spread(s, part, firsts[part] + i * PIECE)
                return carry

            lax.fori_loop(1, (end - firsts[part] + PIECE - 1) // PIECE, more, 0)
        copy(s).start()
        return carry

    lax.fori_loop(0, steps, step, 0)
    for s in range(steps - depth, steps):
        copy(s).wait()


def write_stats(bounds, rows, high, low, total):
    padded, cols = high.shape
    vmem = pl.BlockSpec(memory_space=pltpu.VMEM)
    height = 1024
    depth = min(4, total // height)
    return pl.pallas_call(
        stats_kernel,
        out_shape=jax.ShapeDtypeStruct((total, cols), jnp.float32),
        in_specs=[pl.BlockSpec(memory_space=pltpu.SMEM), vmem, vmem, vmem],
        out_specs=pl.BlockSpec(memory_space=pl.ANY),
        scratch_shapes=[
            pltpu.VMEM(((padded - PIECE) // STEP, PIECE), jnp.int32),
            pltpu.VMEM((depth, height, cols), jnp.float32),
            pltpu.SemaphoreType.DMA((depth,)),
        ],
        compiler_params=pltpu.CompilerParams(vmem_limit_bytes=STATS_LIMIT),
    )(bounds, rows, high, low)


def per_device(log_beta, gamma_init, topic_prior, word_block, word_row, counts):
    doc_rows, length = counts.shape
    vocab = log_beta.shape[0]
    all_docs = lax.axis_size("docs") * doc_rows
    slots = 2 * doc_rows * length

    packed = (word_block[:, :, 0] * vocab + word_row) * 4 + counts
    key = lax.sort(share_tokens(packed, vocab).reshape(-1))[:slots]
    blank = vocab * all_docs * 4
    rows = jnp.minimum(key // (4 * all_docs), vocab - 1)
    docs = (key // 4) % all_docs
    count = jnp.where(key < blank, key % 4, 0).astype(jnp.float32)
    limits = jnp.arange(0, vocab + 1, SUB, dtype=jnp.int32) * (all_docs * 4)
    bounds = jnp.sum(key[None, :] < limits[:, None], axis=1, dtype=jnp.int32)
    lines = jnp.pad(rows.reshape(slots // PIECE, PIECE), ((0, 8), (0, 0)), constant_values=-1)

    found = gather_rows(log_beta, lines, bounds)
    doc_gamma, high, low = run_sweeps(found, docs, count, gamma_init, topic_prior)
    sstats = write_stats(bounds, lines, high, low, vocab)
    return (doc_gamma, sstats)


def solution(mesh):
    in_specs = (
        P("docs", "topics"),
        P("docs", "topics"),
        P("topics"),
        P("docs", None, None),
        P("docs", None),
        P("docs", None),
    )
    out_specs = (P("docs", "topics"), P("docs", "topics"))
    return jax.shard_map(
        per_device, mesh=mesh, in_specs=in_specs, out_specs=out_specs, check_vma=False
    )
```
